32 devices in a mesh: groups: 2 (over y), grid: 4 (over z), row: 2 (over core), rep: 2 (over x).
Axes of the slice: x: 2, y: 2, z: 4, core: 2. Of those that a mesh axis runs over, the one named last changes fastest.
Arguments:
- tokens: bfloat16 [1024, 4096], P(('groups', 'grid', 'rep'), 'row'), parts along dimension 0, may hold values from -40 to 40
- target_tokens: int32 [1024], P('groups'), parts along dimension 0, may hold values from 0 to 31999
- gate_weight: bfloat16 [4096, 14336], P(('row', 'rep'), 'grid'), may hold values from -0.09375 to 0.09375
- up_weight: bfloat16 [4096, 14336], P(('row', 'rep'), 'grid'), may hold values from -0.09375 to 0.09375
- down_weight: bfloat16 [14336, 4096], P('grid', ('row', 'rep')), may hold values from -0.046875 to 0.046875
- norm_gain: float32 [4096], P('row'), may hold values from 0.5 to 1.5
- vocab_weight: bfloat16 [4096, 32000], P('row', ('grid', 'rep')), may hold values from -6 to 6
Outputs:
- mixed: bfloat16 [1024, 4096], P(('groups', 'grid', 'rep'), 'row'), parts along dimension 0
- logprob: float32 [1024], P(('groups', 'grid', 'rep')), parts along dimension 0
The draws below stay inside these ranges and needn't reach their ends.
There are 2 independent parts, one for each index of `groups`. The reference program is written for one: setup_inputs(seed, part) draws one part's arguments, and reference() takes and returns one part's arrays. A program takes and returns all parts, laid end to end along the dimension named above; an argument that names none is the same for every part. Nothing has to cross between parts.
All inputs are finite; a program needn't handle non-finite values.
Results may differ from the reference program's by a relative error of at most 0.0046.
Values may be sent and summed in bfloat16 or wider, within the bound.
A program may use at most 128 MiB of HBM per device.

```python
import math
import jax
import jax.numpy as jnp
import numpy as np
from jax import lax

D = 4096
FF = 14336
V = 32000
TOKENS = 512


def draw_tokens(key, part):
    key_rows = jax.random.fold_in(key, 0)
    key_cols = jax.random.fold_in(key, 1)
    key_base = jax.random.fold_in(key, 2)
    key_pick = jax.random.fold_in(key, 4)
    key_level = jax.random.fold_in(key, 5)
    key_noise = jax.random.fold_in(key, 6)
    key_mix = jax.random.fold_in(key, 7)
    row_scale = jnp.exp(jax.random.uniform(key_rows, (TOKENS, 1), minval=math.log(0.4), maxval=math.log(4.0)))
    column_ramp = jnp.arange(D, dtype=jnp.float32) / D
    column_scale = 0.5 * jnp.exp(math.log(3.0) * column_ramp + jax.random.uniform(key_cols, (D,), minval=-0.2, maxval=0.2))
    base_draw = jnp.clip(jax.random.normal(key_base, (TOKENS, D)), -5.5, 5.5)
    drawn = base_draw * row_scale * column_scale
    aligned_row = jax.random.randint(key_pick, (TOKENS, 1), 0, 12) == 0
    level = jax.random.uniform(key_level, (TOKENS, 1), minval=2.0, maxval=3.0)
    mix_share = jax.random.uniform(key_mix, (TOKENS, 1), minval=0.15, maxval=2.0)
    noise = jnp.clip(jax.random.normal(key_noise, (TOKENS, D)), -5.0, 5.0)
    aligned = level * (1.0 + mix_share * noise)
    return jnp.clip(jnp.where(aligned_row, aligned, drawn), -40.0, 40.0).astype(jnp.bfloat16)


def draw_vocab_weight(key, part):
    key_base, key_scale, key_heavy, key_pair = jax.random.split(key, 4)
    column_ramp = jnp.arange(V, dtype=jnp.float32) / V
    column_scale = (2.5 + column_ramp + jax.random.uniform(key_scale, (V,), minval=-0.3, maxval=0.3)) / math.sqrt(D)
    base_draw = jnp.clip(jax.random.normal(key_base, (D, V)), -5.0, 5.0) * column_scale
    heavy_level = 320.0 / D
    heavy_draw = heavy_level * (1.0 + 0.15 * jnp.clip(jax.random.normal(key_heavy, (D, V)), -4.0, 4.0))
    partner_draw = jnp.roll(heavy_draw, 1, axis=1) + jnp.clip(jax.random.normal(key_pair, (D, V)), -5.0, 5.0) * (1.5 / math.sqrt(D))
    position = jnp.arange(V) % (V // 4)
    base_draw = jnp.where(position == 0, heavy_draw, jnp.where(position == 1, partner_draw, base_draw))
    return jnp.clip(base_draw, -6.0, 6.0).astype(jnp.bfloat16)


def set_ends(drawn, rng, least, high):
    dims = drawn.shape
    spot = [jax.random.randint(jax.random.fold_in(rng, axis), (), 0, dims[axis]) for axis in range(len(dims))]
    drawn = drawn.at[tuple(spot)].set(least)
    longest = dims.index(max(dims))
    spot[longest] = (spot[longest] + 1) % dims[longest]
    return drawn.at[tuple(spot)].set(high)


def steps_of(own_key, extent, cuts, low, high):
    def one(axis_at, blocks):
        heights = jax.random.uniform(jax.random.fold_in(jax.random.fold_in(own_key, 6), axis_at), (blocks,), jnp.float32, low / len(cuts), high / len(cuts))
        return jnp.repeat(jnp.exp(heights), extent[axis_at] // blocks).reshape((-1,) + (1,) * (len(extent) - axis_at - 1))

    loudness = one(*cuts[0])
    for cut in cuts[1:]:
        loudness = loudness * one(*cut)
    return loudness


def cumulative_ranks(amount, skew):
    portions = [(1 << 20) // math.isqrt(rank ** skew) + 1 for rank in range(1, amount + 1)]
    scale = 1 + sum(portions) // (1 << 30)
    return np.cumsum(np.array([max(1, weight // scale) for weight in portions]))


def ranked(stream_key, shape, count, lean):
    table = cumulative_ranks(count, lean)
    pick = jax.random.randint(jax.random.fold_in(stream_key, 1), shape, 0, int(table[count - 1]))
    standing = jnp.searchsorted(jnp.asarray(table, jnp.int32), pick, side="right")
    return jax.random.permutation(jax.random.fold_in(stream_key, 2), count)[standing].astype(jnp.int32)


def scatter_about(key, extent, scale, limit, cuts=(), kind=jnp.bfloat16):
    result = jax.random.normal(key, extent, jnp.float32) * scale
    if len(cuts) > 0:
        result = steps_of(key, extent, cuts, -0.22, 0.18) * result
    return jnp.clip(result, min=-limit, max=limit).astype(kind)


def setup_inputs(seed: int = 0, part: int = 0) -> dict:
    streams_of = jax.random.split(jax.random.key(seed), 8)
    part_keys = jax.random.split(jax.random.fold_in(streams_of[7], part), 8)
    tokens = draw_tokens(jax.random.fold_in(jax.random.fold_in(streams_of[7], part), 71), part)
    target_tokens = set_ends(ranked(part_keys[1], (TOKENS,), V, 2), jax.random.fold_in(part_keys[1], 3), 0, V - 1).astype(jnp.int32)
    gate_weight = scatter_about(streams_of[2], (D, FF), D ** -0.5, 0.09375, ((0, 4), (1, 4)))
    up_weight = scatter_about(streams_of[3], (D, FF), D ** -0.5, 0.09375, ((0, 4), (1, 4)))
    down_weight = scatter_about(streams_of[4], (FF, D), FF ** -0.5, 0.046875, ((0, 4), (1, 4)))
    norm_gain = jnp.clip(1.0 + 0.1 * jax.random.normal(streams_of[5], (D,), jnp.float32), 0.5, 1.5)
    vocab_weight = draw_vocab_weight(jax.random.fold_in(streams_of[7], 71), part)
    return {"tokens": tokens, "target_tokens": target_tokens, "gate_weight": gate_weight, "up_weight": up_weight, "down_weight": down_weight, "norm_gain": norm_gain, "vocab_weight": vocab_weight}


def reference(tokens, target_tokens, gate_weight, up_weight, down_weight, norm_gain, vocab_weight):
    gate_value = jnp.dot(tokens, gate_weight, preferred_element_type=jnp.float32)
    up_value = jnp.dot(tokens, up_weight, preferred_element_type=jnp.float32)
    hidden = (jax.nn.silu(gate_value) * up_value).astype(jnp.bfloat16)
    mixed_full = tokens.astype(jnp.float32) + jnp.dot(hidden, down_weight, preferred_element_type=jnp.float32)
    mixed = mixed_full.astype(jnp.bfloat16)
    held = lax.optimization_barrier(mixed).astype(jnp.float32)
    scale = lax.rsqrt(lax.optimization_barrier(jnp.sum(held * held, axis=1, keepdims=True)) / D + 1e-05)
    normed = (held * scale * norm_gain.astype(jnp.float32)).astype(jnp.bfloat16)
    logits = jnp.dot(normed, vocab_weight, preferred_element_type=jnp.float32)
    row_top = lax.optimization_barrier(jnp.max(logits, axis=1, keepdims=True))
    row_total = lax.optimization_barrier(jnp.sum(jnp.exp(logits - row_top), axis=1))
    picked = jnp.take_along_axis(logits, target_tokens.astype(jnp.int32)[:, None], axis=1)[:, 0]
    logprob = picked - row_top[:, 0] - jnp.log(row_total)
    return (mixed, logprob)
```

```python
import jax
import jax.numpy as jnp
from jax import lax
from jax.sharding import PartitionSpec as P

SWAP = [(0, 1), (1, 0)]
F32 = jnp.float32
BF16 = jnp.bfloat16


def pick_target(logits, targets, column_start):
    column_ids = column_start + lax.broadcasted_iota(jnp.int32, logits.shape, 1)
    return jnp.sum(jnp.where(column_ids == targets[:, None], logits, 0.0), axis=1)


def stats_all(logits, targets, column_start):
    picked = pick_target(logits, targets, column_start)
    row_top = lax.pmax(jnp.max(logits, axis=1), ("grid", "rep"))
    local_total = jnp.sum(jnp.exp(logits - row_top[:, None]), axis=1)
    row_total, target_logit = lax.psum((local_total, picked), ("grid", "rep"))
    return target_logit - row_top - jnp.log(row_total)


def general(tokens, target_tokens, gate_weight, up_weight, down_weight, norm_gain, vocab_weight):
    own_rows = tokens.shape[0]
    width = tokens.shape[1] * lax.axis_size("row")
    copy_rows = lax.all_gather(tokens, "grid", axis=0, tiled=True)
    gate_part = jnp.dot(
        copy_rows,
        lax.all_gather(gate_weight, "rep", axis=0, tiled=True),
        preferred_element_type=F32,
    )
    up_part = jnp.dot(
        copy_rows,
        lax.all_gather(up_weight, "rep", axis=0, tiled=True),
        preferred_element_type=F32,
    )
    gate_value, up_value = lax.psum((gate_part, up_part), "row")
    hidden = (jax.nn.silu(gate_value) * up_value).astype(BF16)
    down_full = lax.all_gather(down_weight, "rep", axis=1, tiled=True)
    branch_sum = lax.psum_scatter(
        jnp.dot(hidden, down_full, preferred_element_type=F32),
        "grid",
        scatter_dimension=0,
        tiled=True,
    )
    mixed = (tokens.astype(F32) + branch_sum).astype(BF16)
    held = lax.optimization_barrier(mixed).astype(F32)
    squares = lax.psum(jnp.sum(held * held, axis=1), "row")
    scale = lax.rsqrt(squares / width + 1e-05)
    normed = (held * scale[:, None] * norm_gain[None, :]).astype(BF16)
    partial_logits = jnp.dot(
        lax.all_gather(normed, ("grid", "rep"), axis=0, tiled=True),
        vocab_weight,
        preferred_element_type=F32,
    )
    logits = lax.psum(partial_logits, "row")
    block_index = lax.axis_index(("grid", "rep"))
    column_start = block_index * vocab_weight.shape[1]
    every_logprob = stats_all(logits, target_tokens, column_start)
    logprob = lax.dynamic_slice_in_dim(every_logprob, block_index * own_rows, own_rows, 0)
    return (mixed, logprob)


def cut(x, which, size, axis=0):
    return lax.dynamic_slice_in_dim(x, which * size, size, axis)


def in_order(me, own, other, axis=0):
    first = jnp.where(me == 0, own, other)
    second = jnp.where(me == 0, other, own)
    return jnp.concatenate([first, second], axis=axis)


def swap(x, axis):
    return lax.ppermute(x, axis, SWAP)


def merge(a, b):
    top = jnp.maximum(a[0], b[0])
    total = a[1] * jnp.exp(a[0] - top) + b[1] * jnp.exp(b[0] - top)
    return jnp.stack([top, total, a[2] + b[2]])


def paired(tokens, target_tokens, gate_weight, up_weight, down_weight, norm_gain, vocab_weight):
    ring = lax.axis_size("grid")
    z = lax.axis_index("grid")
    r = lax.axis_index("row")
    p = lax.axis_index("rep")
    own_rows, half_width = tokens.shape
    width = half_width * 2
    quarter = half_width // 2
    block_rows = own_rows * 2

    def forward(x, k):
        return lax.ppermute(x, "grid", [(i, (i + k) % ring) for i in range(ring)])

    def backward(x, k):
        return lax.ppermute(x, "grid", [(i, (i - k) % ring) for i in range(ring)])

    theirs = swap(cut(tokens, 1 - p, quarter, 1), "rep")
    own_block = in_order(p, cut(tokens, p, quarter, 1), theirs)
    blocks = [own_block] + [forward(own_block, k) for k in range(1, ring)]

    def reduced(x, weight):
        part = jnp.dot(x, weight, preferred_element_type=F32)
        mine = cut(part, r, own_rows) + swap(cut(part, 1 - r, own_rows), "row")
        piece = own_rows // 2
        from_rep = swap(cut(mine, 1 - p, piece).astype(BF16), "rep")
        return cut(mine, p, piece) + from_rep.astype(F32)

    branch = None
    arrivals = []
    for k in range(ring):
        gate_value = reduced(blocks[k], gate_weight)
        up_value = reduced(blocks[k], up_weight)
        hidden = (jax.nn.silu(gate_value) * up_value).astype(BF16)
        hidden = in_order(p, hidden, swap(hidden, "rep"))
        hidden = in_order(r, hidden, swap(hidden, "row"))
        down = jnp.dot(hidden, down_weight, preferred_element_type=F32)
        if k == 0:
            branch = down
        else:
            arrivals.append(backward(down.astype(BF16), k))
    for arrived in arrivals:
        branch = branch + arrived.astype(F32)

    mixed_cols = lax.optimization_barrier((own_block.astype(F32) + branch).astype(BF16))
    column_blocks = [mixed_cols] + [forward(mixed_cols, k) for k in range(1, ring)]
    full_blocks = [in_order(p, c, swap(c, "rep"), 1) for c in column_blocks]
    mixed = cut(full_blocks[0], p, own_rows)

    held = jnp.concatenate(full_blocks, axis=0).astype(F32)
    sums = jnp.sum(held * held, axis=1)
    squares = sums + swap(sums, "row")
    scale = lax.rsqrt(squares / width + 1e-05)
    normed = (held * scale[:, None] * norm_gain[None, :]).astype(BF16)

    half_rows = block_rows * ring // 2
    to_send = jnp.dot(cut(normed, 1 - r, half_rows), vocab_weight, preferred_element_type=F32)
    arrived = swap(to_send, "row")
    logits = jnp.dot(cut(normed, r, half_rows), vocab_weight, preferred_element_type=F32) + arrived
    targets = jnp.concatenate(
        [cut(target_tokens, lax.rem(z - k + ring, ring), block_rows) for k in range(ring)]
    )
    column_start = (z * 2 + p) * vocab_weight.shape[1]
    picked = pick_target(logits, cut(targets, r, half_rows), column_start)
    top = jnp.max(logits, axis=1)
    total = jnp.sum(jnp.exp(logits - top[:, None]), axis=1)
    stats = jnp.stack([top, total, picked])
    stats = in_order(r, stats, swap(stats, "row"), 1)
    result = stats[:, :block_rows]
    returned = [
        backward(stats[:, k * block_rows : (k + 1) * block_rows], k) for k in range(1, ring)
    ]
    for other in returned:
        result = merge(result, other)
    from_rep = swap(cut(result, 1 - p, own_rows, 1), "rep")
    result = merge(cut(result, p, own_rows, 1), from_rep)
    return (mixed, result[2] - result[0] - jnp.log(result[1]))


def solution(mesh):
    in_specs = (
        P(("groups", "grid", "rep"), "row"),
        P("groups"),
        P(("row", "rep"), "grid"),
        P(("row", "rep"), "grid"),
        P("grid", ("row", "rep")),
        P("row"),
        P("row", ("grid", "rep")),
    )
    out_specs = (P(("groups", "grid", "rep"), "row"), P(("groups", "grid", "rep")))
    small = mesh.shape["row"] == 2 and mesh.shape["rep"] == 2 and mesh.shape["grid"] <= 4
    return jax.shard_map(
        paired if small else general,
        mesh=mesh,
        in_specs=in_specs,
        out_specs=out_specs,
        check_vma=False,
    )
```

```python
import jax
import jax.numpy as jnp
from jax import lax
from jax.sharding import PartitionSpec as P

SWAP = [(0, 1), (1, 0)]
F32 = jnp.float32
BF16 = jnp.bfloat16


def pick_target(logits, targets, column_start):
    column_ids = column_start + lax.broadcasted_iota(jnp.int32, logits.shape, 1)
    return jnp.sum(jnp.where(column_ids == targets[:, None], logits, 0.0), axis=1)


def stats_all(logits, targets, column_start):
    picked = pick_target(logits, targets, column_start)
    row_top = lax.pmax(jnp.max(logits, axis=1), ("grid", "rep"))
    local_total = jnp.sum(jnp.exp(logits - row_top[:, None]), axis=1)
    row_total, target_logit = lax.psum((local_total, picked), ("grid", "rep"))
    return target_logit - row_top - jnp.log(row_total)


def general(tokens, target_tokens, gate_weight, up_weight, down_weight, norm_gain, vocab_weight):
    own_rows = tokens.shape[0]
    width = tokens.shape[1] * lax.axis_size("row")
    copy_rows = lax.all_gather(tokens, "grid", axis=0, tiled=True)
    gate_part = jnp.dot(
        copy_rows,
        lax.all_gather(gate_weight, "rep", axis=0, tiled=True),
        preferred_element_type=F32,
    )
    up_part = jnp.dot(
        copy_rows,
        lax.all_gather(up_weight, "rep", axis=0, tiled=True),
        preferred_element_type=F32,
    )
    gate_value, up_value = lax.psum((gate_part, up_part), "row")
    hidden = (jax.nn.silu(gate_value) * up_value).astype(BF16)
    down_full = lax.all_gather(down_weight, "rep", axis=1, tiled=True)
    branch_sum = lax.psum_scatter(
        jnp.dot(hidden, down_full, preferred_element_type=F32),
        "grid",
        scatter_dimension=0,
        tiled=True,
    )
    mixed = (tokens.astype(F32) + branch_sum).astype(BF16)
    held = lax.optimization_barrier(mixed).astype(F32)
    squares = lax.psum(jnp.sum(held * held, axis=1), "row")
    scale = lax.rsqrt(squares / width + 1e-05)
    normed = (held * scale[:, None] * norm_gain[None, :]).astype(BF16)
    partial_logits = jnp.dot(
        lax.all_gather(normed, ("grid", "rep"), axis=0, tiled=True),
        vocab_weight,
        preferred_element_type=F32,
    )
    logits = lax.psum(partial_logits, "row")
    block_index = lax.axis_index(("grid", "rep"))
    column_start = block_index * vocab_weight.shape[1]
    every_logprob = stats_all(logits, target_tokens, column_start)
    logprob = lax.dynamic_slice_in_dim(every_logprob, block_index * own_rows, own_rows, 0)
    return (mixed, logprob)


def cut(x, which, size, axis=0):
    return lax.dynamic_slice_in_dim(x, which * size, size, axis)


def in_order(me, own, other, axis=0):
    first = jnp.where(me == 0, own, other)
    second = jnp.where(me == 0, other, own)
    return jnp.concatenate([first, second], axis=axis)


def swap(x, axis):
    return lax.ppermute(x, axis, SWAP)


def merge(a, b):
    top = jnp.maximum(a[0], b[0])
    total = a[1] * jnp.exp(a[0] - top) + b[1] * jnp.exp(b[0] - top)
    return jnp.stack([top, total, a[2] + b[2]])


def paired(tokens, target_tokens, gate_weight, up_weight, down_weight, norm_gain, vocab_weight):
    ring = lax.axis_size("grid")
    z = lax.axis_index("grid")
    r = lax.axis_index("row")
    p = lax.axis_index("rep")
    own_rows, half_width = tokens.shape
    width = half_width * 2
    quarter = half_width // 2
    block_rows = own_rows * 2

    def forward(x, k):
        return lax.ppermute(x, "grid", [(i, (i + k) % ring) for i in range(ring)])

    def backward(x, k):
        return lax.ppermute(x, "grid", [(i, (i - k) % ring) for i in range(ring)])

    theirs = swap(cut(tokens, 1 - p, quarter, 1), "rep")
    own_block = in_order(p, cut(tokens, p, quarter, 1), theirs)
    blocks = [own_block] + [forward(own_block, k) for k in range(1, ring)]

    piece = own_rows // 2

    def over_row(x, weight):
        part = jnp.dot(x, weight, preferred_element_type=F32)
        mine = cut(part, r, own_rows) + swap(cut(part, 1 - r, own_rows), "row")
        return cut(mine, p, piece), cut(mine, 1 - p, piece).astype(BF16)

    branch = None
    arrivals = []
    for k in range(ring):
        gate_keep, gate_send = over_row(blocks[k], gate_weight)
        up_keep, up_send = over_row(blocks[k], up_weight)
        gate_weight, up_weight, gate_send, up_send = lax.optimization_barrier(
            (gate_weight, up_weight, gate_send, up_send)
        )
        gate_value = gate_keep + swap(gate_send, "rep").astype(F32)
        up_value = up_keep + swap(up_send, "rep").astype(F32)
        hidden = (jax.nn.silu(gate_value) * up_value).astype(BF16)
        hidden = in_order(p, hidden, swap(hidden, "rep"))
        hidden = in_order(r, hidden, swap(hidden, "row"))
        down = jnp.dot(hidden, down_weight, preferred_element_type=F32)
        if k == 0:
            branch = down
        else:
            arrivals.append(backward(down.astype(BF16), k))
    for arrived in arrivals:
        branch = branch + arrived.astype(F32)

    mixed_cols = lax.optimization_barrier((own_block.astype(F32) + branch).astype(BF16))
    column_blocks = [mixed_cols] + [forward(mixed_cols, k) for k in range(1, ring)]
    full_blocks = []
    sums = []
    for c in column_blocks:
        full = lax.optimization_barrier(in_order(p, c, swap(c, "rep"), 1))
        full_blocks.append(full)
        sums.append(jnp.sum(jnp.square(full.astype(F32)), axis=1))
    mixed = cut(full_blocks[0], p, own_rows)
    sums = jnp.concatenate(sums)
    squares = sums + swap(sums, "row")
    scale = lax.rsqrt(squares / width + 1e-05)
    normed = []
    for k, full in enumerate(full_blocks):
        block_scale = scale[k * block_rows : (k + 1) * block_rows, None]
        normed.append((full.astype(F32) * block_scale * norm_gain[None, :]).astype(BF16))
    normed = lax.optimization_barrier(jnp.concatenate(lax.optimization_barrier(normed)))

    half_rows = block_rows * ring // 2
    to_send = jnp.dot(cut(normed, 1 - r, half_rows), vocab_weight, preferred_element_type=F32)
    arrived = swap(to_send, "row")
    kept = jnp.dot(cut(normed, r, half_rows), vocab_weight, preferred_element_type=F32)
    logits = lax.optimization_barrier(kept) + arrived
    targets = jnp.concatenate(
        [cut(target_tokens, lax.rem(z - k + ring, ring), block_rows) for k in range(ring)]
    )
    column_start = (z * 2 + p) * vocab_weight.shape[1]
    picked = pick_target(logits, cut(targets, r, half_rows), column_start)
    top = jnp.max(logits, axis=1)
    total = jnp.sum(jnp.exp(logits - top[:, None]), axis=1)
    stats = jnp.stack([top, total, picked])
    stats = in_order(r, stats, swap(stats, "row"), 1)
    result = stats[:, :block_rows]
    returned = [
        backward(stats[:, k * block_rows : (k + 1) * block_rows], k) for k in range(1, ring)
    ]
    for other in returned:
        result = merge(result, other)
    from_rep = swap(cut(result, 1 - p, own_rows, 1), "rep")
    result = merge(cut(result, p, own_rows, 1), from_rep)
    return (mixed, result[2] - result[0] - jnp.log(result[1]))


def solution(mesh):
    in_specs = (
        P(("groups", "grid", "rep"), "row"),
        P("groups"),
        P(("row", "rep"), "grid"),
        P(("row", "rep"), "grid"),
        P("grid", ("row", "rep")),
        P("row"),
        P("row", ("grid", "rep")),
    )
    out_specs = (P(("groups", "grid", "rep"), "row"), P(("groups", "grid", "rep")))
    small = mesh.shape["row"] == 2 and mesh.shape["rep"] == 2 and mesh.shape["grid"] <= 4
    return jax.shard_map(
        paired if small else general,
        mesh=mesh,
        in_specs=in_specs,
        out_specs=out_specs,
        check_vma=False,
    )
```
